8 devices in a mesh: dp: 1 (over z), sp: 8 (over x, y, core).
Axes of the slice: x: 2, y: 2, z: 1, core: 2. Of those that a mesh axis runs over, the one named last changes fastest.
Arguments:
- x: bfloat16 [4096, 4096], P(('dp', 'sp'))
- gain: bfloat16 [4096], replicated
- wq: bfloat16 [4096, 4096], replicated
- wk: bfloat16 [4096, 4096], replicated
- wv: bfloat16 [4096, 4096], replicated
- wo: bfloat16 [4096, 4096], replicated
Outputs:
- output: bfloat16 [4096, 4096], P(('dp', 'sp'))
All inputs are finite; a program needn't handle non-finite values.
Results may differ from the reference program's by a relative error of at most 0.012.
Values are sent between devices in bfloat16 or wider.
A program may use at most 2 GiB of HBM per device.

```python
import jax
import jax.numpy as jnp
from jax import lax

ROWS = 4096
D = 4096
HEADS = 32
KV_HEADS = 32
HEAD = 128
THETA = 10000


def setup_inputs(seed: int = 0, part: int = 0) -> dict:
    kx, kn, kq, kk, kv, ko = jax.random.split(jax.random.key(seed), 6)

    def weights(key, rows, columns):
        return jax.random.normal(key, (rows, columns), jnp.float32) * rows**-0.5

    drawn = {
        "x": jax.random.normal(jax.random.fold_in(kx, part), (ROWS, D), jnp.float32),
        "gain": 1 + 0.1 * jax.random.normal(kn, (D,), jnp.float32),
        "wq": 2 * weights(kq, D, HEADS * HEAD),
        "wk": 2 * weights(kk, D, KV_HEADS * HEAD),
        "wv": 4 * weights(kv, D, KV_HEADS * HEAD),
        "wo": weights(ko, HEADS * HEAD, D),
    }
    return {k: v.astype(jnp.bfloat16) for k, v in drawn.items()}


def normed(x, gain):
    wide = x.astype(jnp.float32)
    scale = lax.rsqrt(jnp.mean(wide * wide, -1, keepdims=True) + 1e-6)
    return (wide * scale * gain.astype(jnp.float32)).astype(jnp.bfloat16)


def turned(t, place, theta):
    half = t.shape[-1] // 2
    angle = place.astype(jnp.float32)[:, None] * theta ** (-jnp.arange(half, dtype=jnp.float32) / half)
    cos, sin = jnp.cos(angle)[:, None], jnp.sin(angle)[:, None]
    a, b = t[..., :half].astype(jnp.float32), t[..., half:].astype(jnp.float32)
    return jnp.concatenate([a * cos - b * sin, b * cos + a * sin], -1).astype(jnp.bfloat16)


def matmul(a, w):
    return jnp.dot(a, w, preferred_element_type=jnp.float32).astype(jnp.bfloat16)


def einsum(form, a, b):
    return jnp.einsum(form, a.astype(jnp.float32), b.astype(jnp.float32))


def attention(q, k, v):
    scores = einsum("tgsd,ugd->gstu", q, k) * q.shape[-1] ** -0.5
    token = jnp.arange(q.shape[0])
    scores = jnp.where(token[:, None] >= token, scores, -jnp.inf)
    weights = jax.nn.softmax(scores, -1).astype(jnp.bfloat16)
    return einsum("gstu,ugd->tgsd", weights, v).astype(jnp.bfloat16)


def reference(x, gain, wq, wk, wv, wo):
    a, place = normed(x, gain), jnp.arange(ROWS)
    q = turned(matmul(a, wq).reshape(ROWS, HEADS, HEAD), place, THETA).reshape(ROWS, KV_HEADS, -1, HEAD)
    k = turned(matmul(a, wk).reshape(ROWS, KV_HEADS, HEAD), place, THETA)
    v = matmul(a, wv).reshape(ROWS, KV_HEADS, HEAD)
    seen = attention(q, k, v).reshape(ROWS, HEADS * HEAD)
    return (x.astype(jnp.float32) + jnp.dot(seen, wo, preferred_element_type=jnp.float32)).astype(jnp.bfloat16)
```

```python
import functools

import jax
import jax.numpy as jnp
from jax import lax
from jax.experimental import pallas as pl
from jax.experimental.pallas import tpu as pltpu
from jax.sharding import PartitionSpec as P

HEAD = 128
THETA = 10000
NEG = -1e30
HIDDEN = 2 * NEG
LOG2E = 1.4426950408889634
E = HEAD**-0.5 * LOG2E
N_DEV = 8
SLOTS = 4
W = 256
STRIP = 512
MESH = pl.DeviceIdType.MESH


def _dot(a, b, ca, cb):
    return lax.dot_general(a, b, (((ca,), (cb,)), ((), ())), preferred_element_type=jnp.float32)


def _kernel(x_hbm, gain_ref, cos_ref, sin_ref, wq, wk, wv, wo, out_hbm,
            a_s, w_s, stage_s, q_s, k_s, v_s, o_s, mix_s, top_s,
            x_sem, w_sem, swap_send, swap_recv, qkv_send, qkv_recv, o_send, o_recv, out_sem):
    own = x_hbm.shape[0]
    half = own // 2
    dim = x_hbm.shape[1]
    tokens = own * N_DEV
    me = lax.axis_index("sp")
    core = lax.rem(me, 2)
    cy = lax.rem(lax.div(me, 2), 2)
    cx = lax.div(me, 4)
    chip = 2 * cx + cy
    partner = me + 1 - 2 * core
    x_chip, y_chip = 2 * (1 - cx) + cy, 2 * cx + 1 - cy
    x_dev, y_dev = 2 * x_chip + core, 2 * y_chip + core
    weights = (wk, wv, wq)
    outs = (k_s, v_s, q_s)

    chips = (chip, x_chip, y_chip)

    def fetch_w(w, column, slot):
        return pltpu.make_async_copy(w.at[:, pl.ds(pl.multiple_of(column, W), W)], w_s.at[slot], w_sem.at[slot])

    def fetch_qkv(j, n):
        return fetch_w(weights[n // 3], (8 * chips[n % 3] + 2 * j) * HEAD, n % 3)

    x_copy = pltpu.make_async_copy(x_hbm, o_s, x_sem)
    x_copy.start()
    for n in range(3):
        fetch_qkv(0, n).start()

    barrier = pltpu.get_barrier_semaphore()
    for i in range(1, N_DEV):
        pl.semaphore_signal(barrier, inc=1, device_id={"sp": lax.rem(me + i, N_DEV)}, device_id_type=MESH)
    x_copy.wait()
    pl.semaphore_wait(barrier, N_DEV - 1)

    rows = 64

    def swap(i, late):
        at = pl.ds(pl.multiple_of(i * rows + late * half, rows), rows)
        to = pl.ds(pl.multiple_of(own + i * rows + late * half, rows), rows)
        return pltpu.make_async_remote_copy(
            a_s.at[at], a_s.at[to], swap_send.at[late], swap_recv.at[late],
            device_id={"sp": x_dev if late else y_dev}, device_id_type=MESH)

    def norm_piece(i, _):
        for late in range(2):
            at = pl.ds(pl.multiple_of(i * rows + late * half, rows), rows)
            wide = o_s[at, :].astype(jnp.float32)
            scale = lax.rsqrt(jnp.mean(wide * wide, -1, keepdims=True) + 1e-6)
            a_s[at, :] = (wide * scale * gain_ref[...].astype(jnp.float32)).astype(jnp.bfloat16)
            swap(i, late).start()

    lax.fori_loop(0, half // rows, norm_piece, None)

    def bases(p):
        return (me + p * (y_dev - me)) * own, (me + p * (x_dev - me)) * own + half

    def sends(p, j, t, which):
        early, late = bases(p)
        src, dst, sem = stage_s.at[p, j, t], outs[t].at[j], qkv_recv.at[t, j]

        def copy(at, base, device):
            return pltpu.make_async_remote_copy(
                src.at[pl.ds(at, half)], dst.at[pl.ds(pl.multiple_of(base, half), half)], qkv_send, sem,
                device_id={"sp": device}, device_id_type=MESH)

        if which == 0:
            return [copy(0, early, partner), copy(half, late, partner)]
        if which == 1:
            return [copy(own + c * half, early, 2 * x_chip + c) for c in range(2)]
        return [copy(2 * own + c * half, late, 2 * y_chip + c) for c in range(2)]

    def turned(r, at, p, t):
        r = r.astype(jnp.bfloat16)
        parts = []
        for c in range(2):
            b = r[:, c * HEAD : (c + 1) * HEAD]
            if t != 1:
                f = b.astype(jnp.float32)
                here = pl.ds(pl.multiple_of(p * own + at, half), f.shape[0])
                f = f * cos_ref[here, :] + pltpu.roll(f, HEAD // 2, 1) * sin_ref[here, :]
                b = f.astype(jnp.bfloat16)
            parts.append(b)
        return parts

    def project(i, _):
        p, j = lax.div(i, SLOTS), lax.rem(i, SLOTS)
        base = pl.multiple_of(p * own, own)
        early, late = bases(p)

        @pl.when(i == SLOTS)
        def _():
            for n in range(2):
                other = pltpu.make_async_copy(a_s.at[pl.ds(0, half)], a_s.at[pl.ds(own + n * half, half)], swap_recv.at[n])
                other.wait()

        for t in range(3):
            @pl.when((p == 1) & (j > 0))
            def _():
                for which in range(3):
                    for copy in sends(0, j, t, which):
                        copy.start()

            for which in range(3):
                n = 3 * t + which
                fetch_qkv(j, n).wait()
                at, size = (0, own) if which == 0 else ((which - 1) * half, half)
                r = jnp.dot(a_s[pl.ds(pl.multiple_of(base + at, half), size), :], w_s[which], preferred_element_type=jnp.float32)
                low, high = turned(r, at, p, t)
                if which == 0:
                    mine, its = jnp.where(core == 0, low, high), jnp.where(core == 0, high, low)
                    stage_s[p, j, t, :own, :] = its
                    outs[t][j, pl.ds(pl.multiple_of(early, half), half), :] = mine[:half]
                    outs[t][j, pl.ds(pl.multiple_of(late, half), half), :] = mine[half:]
                else:
                    stage_s[p, j, t, which * own : which * own + half, :] = low
                    stage_s[p, j, t, which * own + half : (which + 1) * own, :] = high

                @pl.when((p == 1) | (j == 0))
                def _():
                    for copy in sends(p, j, t, which):
                        copy.start()

                if n < 6:
                    fetch_qkv(j, n + 3).start()
                else:
                    @pl.when(i < 2 * SLOTS - 1)
                    def _():
                        fetch_qkv(lax.rem(j + 1, SLOTS), n - 6).start()

    lax.fori_loop(0, 2 * SLOTS, project, None)

    for late in range(2):
        pltpu.make_async_copy(a_s.at[pl.ds(0, half)], a_s.at[pl.ds(own, half)], swap_send.at[late]).wait()
    x_again = pltpu.make_async_copy(x_hbm, a_s.at[pl.ds(0, own)], x_sem)
    x_again.start()
    for n in range(3):
        fetch_w(wo, n * W, n).start()

    ones = jnp.ones((8, STRIP), jnp.bfloat16)

    def update(work):
        scores = [[_dot(k(), q(), 1, 1) for k, _, _ in blocks] for _, q, blocks in work]
        weights_, keeps = [], []
        for (n, _, blocks), ss in zip(work, scores):
            ss = [s if mask is None else jnp.where(mask, s, HIDDEN) for s, (_, _, mask) in zip(ss, blocks)]
            old = top_s[n : n + 1, :]
            top = old
            for s in ss:
                top = jnp.maximum(top, s.max(axis=0, keepdims=True))
            top_s[n : n + 1, :] = top
            weights_.append([jnp.exp2((s - top) * E).astype(jnp.bfloat16) for s in ss])
            keeps.append(jnp.exp2((old - top) * E))
        for (n, _, blocks), ps, keep in zip(work, weights_, keeps):
            total = mix_s[n] * keep
            for p, (_, v, _) in zip(ps, blocks):
                total = total + _dot(jnp.concatenate([v().T, ones], axis=0), p, 1, 0)
            mix_s[n] = total

    def attend(i, _):
        pair, turn = lax.div(i, 4), lax.rem(i, 4)
        s = 2 * lax.rem(cx + 1 - lax.div(turn, 2), 2) + lax.rem(cy + 1 - lax.rem(turn, 2), 2)
        first = pl.multiple_of(s * 2 * STRIP, 2 * STRIP)

        @pl.when(turn == 0)
        def _():
            for h in range(2):
                for t in range(3):
                    there = outs[t].at[2 * pair + h, pl.ds(0, tokens - 2 * own)]
                    pltpu.make_async_copy(there, there, qkv_recv.at[t, 2 * pair + h]).wait()

        for n in range(4):
            top_s[n : n + 1, :] = jnp.full((1, STRIP), NEG, jnp.float32)
            mix_s[n] = jnp.zeros(mix_s.shape[1:], jnp.float32)

        def read(ref, h, at):
            return lambda: ref[2 * pair + h, pl.ds(pl.multiple_of(at, STRIP), STRIP), :]

        def whole(b, _):
            at = b * 2 * STRIP
            update([(2 * h + st, read(q_s, h, first + st * STRIP),
                     [(read(k_s, h, at + m * STRIP), read(v_s, h, at + m * STRIP), None) for m in range(2)])
                    for h in range(2) for st in range(2)])

        lax.fori_loop(0, s, whole, None)
        seen = lax.broadcasted_iota(jnp.int32, (STRIP, STRIP), 1) >= lax.broadcasted_iota(jnp.int32, (STRIP, STRIP), 0)
        update([(2 * h + st, read(q_s, h, first + st * STRIP),
                 [(read(k_s, h, first + m * STRIP), read(v_s, h, first + m * STRIP), seen if m == st else None) for m in range(st + 1)])
                for h in range(2) for st in range(2)])

        for h in range(2):
            for st in range(2):
                n = 2 * h + st
                o = (mix_s[n, :HEAD, :] * (1 / mix_s[n, HEAD : HEAD + 1, :])).T.astype(jnp.bfloat16)
                at = pl.ds(pl.multiple_of(first + st * STRIP, STRIP), STRIP)
                lanes = pl.ds(pl.multiple_of((8 * chip + 2 * (2 * pair + h) + core) * HEAD, HEAD), HEAD)
                to = 2 * s + st

                @pl.when(to == me)
                def _():
                    o_s[:, lanes] = o

                @pl.when(to != me)
                def _():
                    q_s[2 * pair + h, at, :] = o
                    pltpu.make_async_remote_copy(
                        q_s.at[2 * pair + h, at], o_s.at[:, lanes], o_send, o_recv,
                        device_id={"sp": to}, device_id_type=MESH).start()

    lax.fori_loop(0, 8, attend, None)

    x_again.wait()
    back = o_s.at[:, pl.ds(0, dim - dim // N_DEV)]
    pltpu.make_async_copy(back, back, o_recv).wait()
    tiles = dim // W

    def out_copy(n):
        lanes = pl.ds(pl.multiple_of(n * W, W), W)
        return pltpu.make_async_copy(a_s.at[pl.ds(own, own), lanes], out_hbm.at[:, lanes], out_sem)

    def finish(n, _):
        slot = lax.rem(n, 3)
        lanes = pl.ds(pl.multiple_of(n * W, W), W)
        fetch_w(wo, n * W, slot).wait()
        y = jnp.dot(o_s[...], w_s[slot], preferred_element_type=jnp.float32)
        a_s[pl.ds(own, own), lanes] = (a_s[pl.ds(0, own), lanes].astype(jnp.float32) + y).astype(jnp.bfloat16)
        out_copy(n).start()

        @pl.when(n + 3 < tiles)
        def _():
            fetch_w(wo, (n + 3) * W, slot).start()

    lax.fori_loop(0, tiles, finish, None)
    pltpu.make_async_copy(a_s.at[pl.ds(own, own)], out_hbm, out_sem).wait()
    pltpu.make_async_copy(stage_s, stage_s, qkv_send).wait()
    sent = q_s.at[:, pl.ds(0, tokens - own)]
    pltpu.make_async_copy(sent, sent, o_send).wait()


def solution(mesh):
    def step(x, gain, wq, wk, wv, wo):
        own, dim = x.shape
        me = lax.axis_index("sp")
        x_dev, y_dev = lax.rem(me + 4, 8), me + 2 - 4 * lax.rem(lax.div(me, 2), 2)
        half = jnp.arange(own // 2)
        place = jnp.concatenate([me * own + jnp.arange(own), y_dev * own + half, x_dev * own + own // 2 + half])
        angle = place.astype(jnp.float32)[:, None] * THETA ** (-jnp.arange(HEAD // 2, dtype=jnp.float32) / (HEAD // 2))
        cos, sin = jnp.cos(angle), jnp.sin(angle)
        cos, sin = jnp.concatenate([cos, cos], 1), jnp.concatenate([-sin, sin], 1)
        tokens = own * N_DEV
        any_, vmem = pl.BlockSpec(memory_space=pl.ANY), pl.BlockSpec(memory_space=pltpu.VMEM)
        bf16, f32 = jnp.bfloat16, jnp.float32
        dma = pltpu.SemaphoreType.DMA
        heads = pltpu.VMEM((SLOTS, tokens, HEAD), bf16)
        return pl.pallas_call(
            _kernel,
            out_shape=jax.ShapeDtypeStruct((own, dim), bf16),
            in_specs=[any_, vmem, vmem, vmem, any_, any_, any_, any_],
            out_specs=any_,
            scratch_shapes=[
                pltpu.VMEM((2 * own, dim), bf16),
                pltpu.VMEM((3, dim, W), bf16),
                pltpu.VMEM((2, SLOTS, 3, 3 * own, HEAD), bf16),
                heads, heads, heads,
                pltpu.VMEM((own, dim), bf16),
                pltpu.VMEM((4, HEAD + 8, STRIP), f32),
                pltpu.VMEM((8, STRIP), f32),
                dma, dma((3,)), dma((2,)), dma((2,)), dma, dma((3, SLOTS)), dma, dma, dma,
            ],
            compiler_params=pltpu.CompilerParams(collective_id=0, has_side_effects=True, vmem_limit_bytes=67043328),
        )(x, gain.reshape(1, dim), cos, sin, wq, wk, wv, wo)

    tokens, whole = P(("dp", "sp"), None), P(None, None)
    return jax.shard_map(
        step,
        mesh=mesh,
        in_specs=(tokens, P(None), whole, whole, whole, whole),
        out_specs=tokens,
        check_vma=False,
    )
```

```python
import jax
import jax.numpy as jnp
import numpy as np
from jax import lax
from jax.experimental import pallas as pl
from jax.experimental.pallas import tpu as pltpu
from jax.sharding import PartitionSpec as P

HEAD = 128
THETA = 10000
NEG = -1e30
HIDDEN = 2 * NEG
LOG2E = 1.4426950408889634
E = HEAD**-0.5 * LOG2E
N_DEV = 8
SLOTS = 4
W = 256
STRIP = 512
MESH = pl.DeviceIdType.MESH


def _dot(a, b, ca, cb):
    return lax.dot_general(a, b, (((ca,), (cb,)), ((), ())), preferred_element_type=jnp.float32)


def _kernel(x_hbm, gain_ref, wq, wk, wv, wo, out_hbm,
            cos_ref, sin_ref, a_s, w_s, r_s, stage_s, q_s, k_s, v_s, o_s, mix_s, top_s,
            x_sem, w_sem, swap_send, swap_recv, qkv_send, qkv_recv, o_send, o_recv, out_sem):
    own = x_hbm.shape[0]
    half = own // 2
    dim = x_hbm.shape[1]
    tokens = own * N_DEV
    me = lax.axis_index("sp")
    core = lax.rem(me, 2)
    cy = lax.rem(lax.div(me, 2), 2)
    cx = lax.div(me, 4)
    chip = 2 * cx + cy
    partner = me + 1 - 2 * core
    x_chip, y_chip = 2 * (1 - cx) + cy, 2 * cx + 1 - cy
    x_dev, y_dev = 2 * x_chip + core, 2 * y_chip + core
    weights = (wk, wv, wq)
    outs = (k_s, v_s, q_s)

    chips = (chip, x_chip, y_chip)

    def fetch_w(w, column, here, sem):
        return pltpu.make_async_copy(w.at[:, pl.ds(pl.multiple_of(column, W), W)], here, sem)

    def fetch_step(j, t, bank):
        return [fetch_w(weights[t], (8 * chips[n] + 2 * j) * HEAD, w_s.at[bank, n], w_sem.at[bank, n]) for n in range(3)]

    rows = 64

    def x_piece(i, late):
        at = pl.ds(pl.multiple_of(i * rows + late * half, rows), rows)
        return pltpu.make_async_copy(x_hbm.at[at], o_s.at[at], x_sem.at[i, late])

    for i in range(half // rows):
        for late in range(2):
            x_piece(i, late).start()
    barrier = pltpu.get_barrier_semaphore()
    for i in range(1, N_DEV):
        pl.semaphore_signal(barrier, inc=1, device_id={"sp": lax.rem(me + i, N_DEV)}, device_id_type=MESH)
    pl.semaphore_wait(barrier, N_DEV - 1)

    def swap(i, late):
        at = pl.ds(pl.multiple_of(i * rows + late * half, rows), rows)
        to = pl.ds(pl.multiple_of(own + i * rows + late * half, rows), rows)
        return pltpu.make_async_remote_copy(
            a_s.at[at], a_s.at[to], swap_send.at[late], swap_recv.at[late],
            device_id={"sp": x_dev if late else y_dev}, device_id_type=MESH)

    def norm_piece(i, _):
        for late in range(2):
            at = pl.ds(pl.multiple_of(i * rows + late * half, rows), rows)
            x_piece(i, late).wait()
            wide = o_s[at, :].astype(jnp.float32)
            scale = lax.rsqrt(jnp.mean(wide * wide, -1, keepdims=True) + 1e-6)
            a_s[at, :] = (wide * scale * gain_ref[...].astype(jnp.float32).reshape(1, dim)).astype(jnp.bfloat16)
            swap(i, late).start()

    lax.fori_loop(0, half // rows, norm_piece, None)
    for t in range(2):
        for copy in fetch_step(0, t, t):
            copy.start()

    lane = lax.rem(lax.broadcasted_iota(jnp.int32, (8, HEAD), 1), HEAD // 2)
    rate = jnp.zeros((8, HEAD), jnp.float32)
    for n in range(HEAD // 2):
        rate = jnp.where(lane == n, np.float32(THETA ** (-n / (HEAD // 2))), rate)
    sign = jnp.where(lax.broadcasted_iota(jnp.int32, (8, HEAD), 1) < HEAD // 2, -1.0, 1.0)

    def factors(i, _):
        at = i * HEAD
        first = jnp.where(at < own, me * own + at, jnp.where(at < own + half, y_dev * own + at - own, x_dev * own + at - own))
        place = (first + lax.broadcasted_iota(jnp.int32, (HEAD, HEAD), 0)).astype(jnp.float32)
        angle = place * rate[:1]
        here = pl.ds(pl.multiple_of(at, HEAD), HEAD)
        cos_ref[here, :] = jnp.cos(angle)
        sin_ref[here, :] = jnp.sin(angle) * sign[:1]

    lax.fori_loop(0, 2 * own // HEAD, factors, None)

    def bases(p):
        return (me + p * (y_dev - me)) * own, (me + p * (x_dev - me)) * own + half

    def sends(p, j, t, which):
        early, late = bases(p)
        src, dst, sem = stage_s.at[p, j, t], outs[t].at[j], qkv_recv.at[t, j]

        def copy(at, base, device):
            return pltpu.make_async_remote_copy(
                src.at[pl.ds(at, half)], dst.at[pl.ds(pl.multiple_of(base, half), half)], qkv_send, sem,
                device_id={"sp": device}, device_id_type=MESH)

        if which == 0:
            return [copy(0, early, partner), copy(half, late, partner)]
        if which == 1:
            return [copy(own + c * half, early, 2 * x_chip + c) for c in range(2)]
        return [copy(2 * own + c * half, late, 2 * y_chip + c) for c in range(2)]

    def turned(r, at, p, t):
        r = r.astype(jnp.bfloat16)
        if t == 1:
            return r
        f = r.astype(jnp.float32)
        here = pl.ds(pl.multiple_of(p * own + at, half), f.shape[0])
        return (f * cos_ref[here, :] + pltpu.roll(f, HEAD // 2, 1) * sin_ref[here, :]).astype(jnp.bfloat16)

    def settle(p, j, t):
        early, late = bases(p)
        low, high = (turned(r_s[t, :own, c * HEAD : (c + 1) * HEAD], 0, p, t) for c in range(2))
        mine, its = jnp.where(core == 0, low, high), jnp.where(core == 0, high, low)
        stage_s[p, j, t, :own, :] = its
        outs[t][j, pl.ds(pl.multiple_of(early, half), half), :] = mine[:half]
        outs[t][j, pl.ds(pl.multiple_of(late, half), half), :] = mine[half:]
        for n in range(2):
            for c in range(2):
                at = (n + 1) * own + c * half
                r = r_s[t, own + n * half : own + (n + 1) * half, c * HEAD : (c + 1) * HEAD]
                stage_s[p, j, t, at : at + half, :] = turned(r, n * half, p, t)

    def send(p, j, t):
        for which in range(3):
            for copy in sends(p, j, t, which):
                copy.start()

    def project(i, _):
        p, j = lax.div(i, SLOTS), lax.rem(i, SLOTS)
        base = pl.multiple_of(p * own, own)

        @pl.when(i == SLOTS)
        def _():
            for n in range(2):
                other = pltpu.make_async_copy(a_s.at[pl.ds(0, half)], a_s.at[pl.ds(own + n * half, half)], swap_recv.at[n])
                other.wait()

        for t in range(3):
            bank = lax.rem(i + t, 2)
            for copy in fetch_step(j, t, bank):
                copy.wait()
            before = jnp.maximum(i - 1, 0) if t == 0 else i
            old = lax.div(before, SLOTS), lax.rem(before, SLOTS), (t + 2) % 3
            settle(*old)
            for n in range(3):
                at, size = (0, own) if n == 0 else ((n - 1) * half, half)
                to = 0 if n == 0 else own + (n - 1) * half
                r_s[t, to : to + size, :] = jnp.dot(
                    a_s[pl.ds(pl.multiple_of(base + at, half), size), :], w_s[bank, n], preferred_element_type=jnp.float32)

            fresh = (old[0] == 1) | (old[1] == 0)

            @pl.when(fresh & (i > 0) if t == 0 else fresh)
            def _():
                send(*old)

            @pl.when((p == 1) & (j > 0))
            def _():
                send(0, j, t)

            ahead = i if t == 0 else i + 1

            @pl.when(ahead < 2 * SLOTS)
            def _():
                for copy in fetch_step(lax.rem(ahead, SLOTS), (t + 2) % 3, bank):
                    copy.start()

    lax.fori_loop(0, 2 * SLOTS, project, None)
    settle(1, SLOTS - 1, 2)
    send(1, SLOTS - 1, 2)

    for late in range(2):
        pltpu.make_async_copy(a_s.at[pl.ds(0, half)], a_s.at[pl.ds(own, half)], swap_send.at[late]).wait()
    x_again = pltpu.make_async_copy(x_hbm, a_s.at[pl.ds(0, own)], x_sem.at[0, 0])
    x_again.start()

    def fetch_wo(n, slot):
        return fetch_w(wo, n * W, w_s.at[lax.div(slot, 3), lax.rem(slot, 3)], w_sem.at[lax.div(slot, 3), lax.rem(slot, 3)])

    for n in range(6):
        fetch_wo(n, n).start()

    ones = jnp.ones((8, STRIP), jnp.bfloat16)

    def update(work):
        scores = [[_dot(k(), q(), 1, 1) for k, _, _ in blocks] for _, q, blocks in work]
        weights_, keeps = [], []
        for (n, _, blocks), ss in zip(work, scores):
            ss = [s if mask is None else jnp.where(mask, s, HIDDEN) for s, (_, _, mask) in zip(ss, blocks)]
            old = top_s[n : n + 1, :]
            top = old
            for s in ss:
                top = jnp.maximum(top, s.max(axis=0, keepdims=True))
            top_s[n : n + 1, :] = top
            weights_.append([jnp.exp2((s - top) * E).astype(jnp.bfloat16) for s in ss])
            keeps.append(jnp.exp2((old - top) * E))
        for (n, _, blocks), ps, keep in zip(work, weights_, keeps):
            total = mix_s[n] * keep
            for p, (_, v, _) in zip(ps, blocks):
                total = total + _dot(jnp.concatenate([v().T, ones], axis=0), p, 1, 0)
            mix_s[n] = total

    def attend(i, _):
        pair, turn = lax.div(i, 4), lax.rem(i, 4)
        s = 2 * lax.rem(cx + 1 - lax.div(turn, 2), 2) + lax.rem(cy + 1 - lax.rem(turn, 2), 2)
        first = pl.multiple_of(s * 2 * STRIP, 2 * STRIP)

        @pl.when(turn == 0)
        def _():
            for h in range(2):
                for t in range(3):
                    there = outs[t].at[2 * pair + h, pl.ds(0, tokens - 2 * own)]
                    pltpu.make_async_copy(there, there, qkv_recv.at[t, 2 * pair + h]).wait()

        for n in range(4):
            top_s[n : n + 1, :] = jnp.full((1, STRIP), NEG, jnp.float32)
            mix_s[n] = jnp.zeros(mix_s.shape[1:], jnp.float32)

        def read(ref, h, at):
            return lambda: ref[2 * pair + h, pl.ds(pl.multiple_of(at, STRIP), STRIP), :]

        def whole(b, _):
            at = b * 2 * STRIP
            update([(2 * h + st, read(q_s, h, first + st * STRIP),
                     [(read(k_s, h, at + m * STRIP), read(v_s, h, at + m * STRIP), None) for m in range(2)])
                    for h in range(2) for st in range(2)])

        lax.fori_loop(0, s, whole, None)
        seen = lax.broadcasted_iota(jnp.int32, (STRIP, STRIP), 1) >= lax.broadcasted_iota(jnp.int32, (STRIP, STRIP), 0)
        update([(2 * h + st, read(q_s, h, first + st * STRIP),
                 [(read(k_s, h, first + m * STRIP), read(v_s, h, first + m * STRIP), seen if m == st else None) for m in range(st + 1)])
                for h in range(2) for st in range(2)])

        for h in range(2):
            for st in range(2):
                n = 2 * h + st
                o = (mix_s[n, :HEAD, :] * (1 / mix_s[n, HEAD : HEAD + 1, :])).T.astype(jnp.bfloat16)
                at = pl.ds(pl.multiple_of(first + st * STRIP, STRIP), STRIP)
                lanes = pl.ds(pl.multiple_of((8 * chip + 2 * (2 * pair + h) + core) * HEAD, HEAD), HEAD)
                to = 2 * s + st

                @pl.when(to == me)
                def _():
                    o_s[:, lanes] = o

                @pl.when(to != me)
                def _():
                    q_s[2 * pair + h, at, :] = o
                    pltpu.make_async_remote_copy(
                        q_s.at[2 * pair + h, at], o_s.at[:, lanes], o_send, o_recv,
                        device_id={"sp": to}, device_id_type=MESH).start()

    lax.fori_loop(0, 8, attend, None)

    x_again.wait()
    back = o_s.at[:, pl.ds(0, dim - dim // N_DEV)]
    pltpu.make_async_copy(back, back, o_recv).wait()
    tiles = dim // W

    def out_copy(n):
        lanes = pl.ds(pl.multiple_of(n * W, W), W)
        return pltpu.make_async_copy(a_s.at[pl.ds(own, own), lanes], out_hbm.at[:, lanes], out_sem)

    def finish(n, _):
        slot = lax.rem(n, 6)
        lanes = pl.ds(pl.multiple_of(n * W, W), W)
        fetch_wo(n, slot).wait()
        y = jnp.dot(o_s[...], w_s[lax.div(slot, 3), lax.rem(slot, 3)], preferred_element_type=jnp.float32)
        a_s[pl.ds(own, own), lanes] = (a_s[pl.ds(0, own), lanes].astype(jnp.float32) + y).astype(jnp.bfloat16)
        out_copy(n).start()

        @pl.when(n + 6 < tiles)
        def _():
            fetch_wo(n + 6, slot).start()

    lax.fori_loop(0, tiles, finish, None)
    pltpu.make_async_copy(a_s.at[pl.ds(own, own)], out_hbm, out_sem).wait()
    pltpu.make_async_copy(stage_s, stage_s, qkv_send).wait()
    sent = q_s.at[:, pl.ds(0, tokens - own)]
    pltpu.make_async_copy(sent, sent, o_send).wait()


def solution(mesh):
    def step(x, gain, wq, wk, wv, wo):
        own, dim = x.shape
        tokens = own * N_DEV
        any_, vmem = pl.BlockSpec(memory_space=pl.ANY), pl.BlockSpec(memory_space=pltpu.VMEM)
        bf16, f32 = jnp.bfloat16, jnp.float32
        dma = pltpu.SemaphoreType.DMA
        heads = pltpu.VMEM((SLOTS, tokens, HEAD), bf16)
        return pl.pallas_call(
            _kernel,
            out_shape=jax.ShapeDtypeStruct((own, dim), bf16),
            in_specs=[any_, vmem, any_, any_, any_, any_],
            out_specs=any_,
            scratch_shapes=[
                pltpu.VMEM((2 * own, HEAD), f32),
                pltpu.VMEM((2 * own, HEAD), f32),
                pltpu.VMEM((2 * own, dim), bf16),
                pltpu.VMEM((2, 3, dim, W), bf16),
                pltpu.VMEM((3, 2 * own, W), f32),
                pltpu.VMEM((2, SLOTS, 3, 3 * own, HEAD), bf16),
                heads, heads, heads,
                pltpu.VMEM((own, dim), bf16),
                pltpu.VMEM((4, HEAD + 8, STRIP), f32),
                pltpu.VMEM((8, STRIP), f32),
                dma((4, 2)), dma((2, 3)), dma((2,)), dma((2,)), dma, dma((3, SLOTS)), dma, dma, dma,
            ],
            compiler_params=pltpu.CompilerParams(collective_id=0, has_side_effects=True, vmem_limit_bytes=67043328),
        )(x, gain, wq, wk, wv, wo)

    tokens, whole = P(("dp", "sp"), None), P(None, None)
    return jax.shard_map(
        step,
        mesh=mesh,
        in_specs=(tokens, P(None), whole, whole, whole, whole),
        out_specs=tokens,
        check_vma=False,
    )
```

```python
import jax
import jax.numpy as jnp
import numpy as np
from jax import lax
from jax.experimental import pallas as pl
from jax.experimental.pallas import tpu as pltpu
from jax.sharding import PartitionSpec as P

HEAD = 128
THETA = 10000
NEG = -1e30
HIDDEN = 2 * NEG
LOG2E = 1.4426950408889634
E = HEAD**-0.5 * LOG2E
N_DEV = 8
SLOTS = 4
W = 256
STRIP = 512
AHEAD = 1
MESH = pl.DeviceIdType.MESH


def _dot(a, b, ca, cb):
    return lax.dot_general(a, b, (((ca,), (cb,)), ((), ())), preferred_element_type=jnp.float32)


def _kernel(x_hbm, gain_ref, wq, wk, wv, wo, out_hbm,
            cos_ref, sin_ref, a_s, w_s, r_s, stage_s, q_s, k_s, v_s, o_s, mix_s, top_s,
            x_sem, w_sem, swap_send, swap_recv, qkv_send, qkv_recv, o_send, o_recv, out_sem):
    own = x_hbm.shape[0]
    half = own // 2
    dim = x_hbm.shape[1]
    tokens = own * N_DEV
    me = lax.axis_index("sp")
    core = lax.rem(me, 2)
    cy = lax.rem(lax.div(me, 2), 2)
    cx = lax.div(me, 4)
    chip = 2 * cx + cy
    partner = me + 1 - 2 * core
    x_chip, y_chip = 2 * (1 - cx) + cy, 2 * cx + 1 - cy
    x_dev, y_dev = 2 * x_chip + core, 2 * y_chip + core
    weights = (wk, wv, wq)
    outs = (k_s, v_s, q_s)

    chips = (chip, x_chip, y_chip)

    def fetch_w(w, column, here, sem):
        return pltpu.make_async_copy(w.at[:, pl.ds(pl.multiple_of(column, W), W)], here, sem)

    def fetch_step(j, t, bank):
        return [fetch_w(weights[t], (8 * chips[n] + 2 * j) * HEAD, w_s.at[bank, n], w_sem.at[bank, n]) for n in range(3)]

    rows = 64

    def x_piece(i, late):
        at = pl.ds(pl.multiple_of(i * rows + late * half, rows), rows)
        return pltpu.make_async_copy(x_hbm.at[at], o_s.at[at], x_sem.at[i, late])

    for i in range(half // rows):
        for late in range(2):
            x_piece(i, late).start()
    barrier = pltpu.get_barrier_semaphore()
    for i in range(1, N_DEV):
        pl.semaphore_signal(barrier, inc=1, device_id={"sp": lax.rem(me + i, N_DEV)}, device_id_type=MESH)
    pl.semaphore_wait(barrier, N_DEV - 1)

    def swap(i, late):
        at = pl.ds(pl.multiple_of(i * rows + late * half, rows), rows)
        to = pl.ds(pl.multiple_of(own + i * rows + late * half, rows), rows)
        return pltpu.make_async_remote_copy(
            a_s.at[at], a_s.at[to], swap_send.at[late], swap_recv.at[late],
            device_id={"sp": x_dev if late else y_dev}, device_id_type=MESH)

    def norm_piece(i, _):
        for late in range(2):
            at = pl.ds(pl.multiple_of(i * rows + late * half, rows), rows)
            x_piece(i, late).wait()
            wide = o_s[at, :].astype(jnp.float32)
            scale = lax.rsqrt(jnp.mean(wide * wide, -1, keepdims=True) + 1e-6)
            a_s[at, :] = (wide * scale * gain_ref[...].astype(jnp.float32).reshape(1, dim)).astype(jnp.bfloat16)
            swap(i, late).start()

    lax.fori_loop(0, half // rows, norm_piece, None)
    for t in range(2):
        for copy in fetch_step(0, t, t):
            copy.start()

    lane = lax.rem(lax.broadcasted_iota(jnp.int32, (8, HEAD), 1), HEAD // 2)
    rate = jnp.zeros((8, HEAD), jnp.float32)
    for n in range(HEAD // 2):
        rate = jnp.where(lane == n, np.float32(THETA ** (-n / (HEAD // 2))), rate)
    sign = jnp.where(lax.broadcasted_iota(jnp.int32, (8, HEAD), 1) < HEAD // 2, -1.0, 1.0)

    def factors(i, _):
        at = i * HEAD
        first = jnp.where(at < own, me * own + at, jnp.where(at < own + half, y_dev * own + at - own, x_dev * own + at - own))
        place = (first + lax.broadcasted_iota(jnp.int32, (HEAD, HEAD), 0)).astype(jnp.float32)
        angle = place * rate[:1]
        here = pl.ds(pl.multiple_of(at, HEAD), HEAD)
        cos_ref[here, :] = jnp.cos(angle)
        sin_ref[here, :] = jnp.sin(angle) * sign[:1]

    lax.fori_loop(0, 2 * own // HEAD, factors, None)

    def bases(p):
        return (me + p * (y_dev - me)) * own, (me + p * (x_dev - me)) * own + half

    def sends(p, j, t, which):
        early, late = bases(p)
        src, dst, sem = stage_s.at[p, j, t], outs[t].at[j], qkv_recv.at[t, j]

        def copy(at, base, device):
            return pltpu.make_async_remote_copy(
                src.at[pl.ds(at, half)], dst.at[pl.ds(pl.multiple_of(base, half), half)], qkv_send, sem,
                device_id={"sp": device}, device_id_type=MESH)

        if which == 0:
            return [copy(0, early, partner), copy(half, late, partner)]
        if which == 1:
            return [copy(own + c * half, early, 2 * x_chip + c) for c in range(2)]
        return [copy(2 * own + c * half, late, 2 * y_chip + c) for c in range(2)]

    def turned(r, at, p, t):
        r = r.astype(jnp.bfloat16)
        if t == 1:
            return r
        f = r.astype(jnp.float32)
        here = pl.ds(pl.multiple_of(p * own + at, half), f.shape[0])
        return (f * cos_ref[here, :] + pltpu.roll(f, HEAD // 2, 1) * sin_ref[here, :]).astype(jnp.bfloat16)

    def settle(p, j, t):
        early, late = bases(p)
        low, high = (turned(r_s[2 * t, :, c * HEAD : (c + 1) * HEAD], 0, p, t) for c in range(2))
        mine, its = jnp.where(core == 0, low, high), jnp.where(core == 0, high, low)
        stage_s[p, j, t, :own, :] = its
        outs[t][j, pl.ds(pl.multiple_of(early, half), half), :] = mine[:half]
        outs[t][j, pl.ds(pl.multiple_of(late, half), half), :] = mine[half:]
        for n in range(2):
            for c in range(2):
                at = (n + 1) * own + c * half
                r = r_s[2 * t + 1, n * half : (n + 1) * half, c * HEAD : (c + 1) * HEAD]
                stage_s[p, j, t, at : at + half, :] = turned(r, n * half, p, t)

    def send(p, j, t):
        for which in range(3):
            for copy in sends(p, j, t, which):
                copy.start()

    def project(i, _):
        p, j = lax.div(i, SLOTS), lax.rem(i, SLOTS)
        base = pl.multiple_of(p * own, own)

        @pl.when(i == SLOTS)
        def _():
            for n in range(2):
                other = pltpu.make_async_copy(a_s.at[pl.ds(0, half)], a_s.at[pl.ds(own + n * half, half)], swap_recv.at[n])
                other.wait()

        for t in range(3):
            bank = lax.rem(i + t, 2)
            for copy in fetch_step(j, t, bank):
                copy.wait()
            before = jnp.maximum(i - 1, 0) if t == 0 else i
            old = lax.div(before, SLOTS), lax.rem(before, SLOTS), (t + 2) % 3
            settle(*old)
            for n in range(3):
                at, size = (0, own) if n == 0 else ((n - 1) * half, half)
                r_s[2 * t + min(n, 1), at : at + size, :] = jnp.dot(
                    a_s[pl.ds(pl.multiple_of(base + at, half), size), :], w_s[bank, n], preferred_element_type=jnp.float32)

            fresh = (old[0] == 1) | (old[1] == 0)

            @pl.when(fresh & (i > 0) if t == 0 else fresh)
            def _():
                send(*old)

            @pl.when((p == 1) & (j > 0))
            def _():
                send(0, j, t)

            ahead = i if t == 0 else i + 1

            @pl.when(ahead < 2 * SLOTS)
            def _():
                for copy in fetch_step(lax.rem(ahead, SLOTS), (t + 2) % 3, bank):
                    copy.start()

    lax.fori_loop(0, 2 * SLOTS, project, None)
    settle(1, SLOTS - 1, 2)
    send(1, SLOTS - 1, 2)

    for late in range(2):
        pltpu.make_async_copy(a_s.at[pl.ds(0, half)], a_s.at[pl.ds(own, half)], swap_send.at[late]).wait()
    x_again = pltpu.make_async_copy(x_hbm, a_s.at[pl.ds(0, own)], x_sem.at[0, 0])
    x_again.start()

    diagonal = 2 * (1 - cx) + 1 - cy
    pieces = ((diagonal, 0), (diagonal, 1), (chip, 0), (chip, 1), (y_chip, 0), (x_chip, 0), (y_chip, 1), (x_chip, 1))
    group = 2 * HEAD
    parts = ((0, range(8)), (8 * group, range(6)), (14 * group, range(6, 8)))
    tiles = dim // W
    wides = [dim // (len(p) * group) for _, p in parts]
    starts = [sum(tiles // w for w in wides[:n]) for n in range(4)]

    def wo_tile(n):
        slot = lax.rem(n, 6)
        return lax.div(slot, 3), lax.rem(slot, 3)

    def start_wo(n, part):
        bank, at = wo_tile(n)
        wide, own_pieces = wides[part], parts[part][1]
        for c in range(wide):
            for m, piece in enumerate(own_pieces):
                row = (pieces[piece][0] * 4 + min(part, 1) * 2 + pieces[piece][1]) * group
                column = ((n - starts[part]) * wide + c) * W
                pltpu.make_async_copy(
                    wo.at[pl.ds(pl.multiple_of(row, group), group), pl.ds(pl.multiple_of(column, W), W)],
                    w_s.at[bank, at, pl.ds((c * len(own_pieces) + m) * group, group)], w_sem.at[bank, at]).start()

    for n in range(6):
        start_wo(n, 0)

    ones = jnp.ones((8, STRIP), jnp.bfloat16)

    def update(work):
        scores = {}

        def score(n):
            if n < len(work):
                scores[n] = [_dot(k(), work[n][1](), 1, 1) for k, _, _ in work[n][2]]

        for n in range(AHEAD):
            score(n)
        for i, (n, _, blocks) in enumerate(work):
            score(i + AHEAD)
            ss = [s if mask is None else jnp.where(mask, s, HIDDEN) for s, (_, _, mask) in zip(scores.pop(i), blocks)]
            old = top_s[n : n + 1, :]
            top = old
            for s in ss:
                top = jnp.maximum(top, s.max(axis=0, keepdims=True))
            top_s[n : n + 1, :] = top
            total = mix_s[n] * jnp.exp2((old - top) * E)
            for s, (_, v, _) in zip(ss, blocks):
                total = total + _dot(jnp.concatenate([v().T, ones], axis=0), jnp.exp2((s - top) * E).astype(jnp.bfloat16), 1, 0)
            mix_s[n] = total

    def chip_at(turn):
        return 2 * lax.rem(cx + 1 - lax.div(turn, 2), 2) + lax.rem(cy + 1 - lax.rem(turn, 2), 2)

    def piece_of(turn, h):
        return jnp.where(turn == 0, h, jnp.where(turn == 3, 2 + h, jnp.where(turn == 2, 4 + 2 * h, 5 + 2 * h)))

    def place(pair, turn, h):
        return pl.ds(pl.multiple_of(((pair * 8 + piece_of(turn, h)) * 2 + core) * HEAD, HEAD), HEAD)

    def give(pair, turn):
        s = chip_at(turn)
        for h in range(2):
            for st in range(2):
                to = 2 * s + st

                @pl.when(to != me)
                def _():
                    pltpu.make_async_remote_copy(
                        q_s.at[2 * pair + h, pl.ds(pl.multiple_of(to * own, own), own)], o_s.at[:, place(pair, turn, h)],
                        o_send, o_recv.at[pair, piece_of(turn, h)], device_id={"sp": to}, device_id_type=MESH).start()

    def attend(i, _):
        pair, turn = lax.div(i, 4), lax.rem(i, 4)
        s = chip_at(turn)
        first = pl.multiple_of(s * 2 * STRIP, 2 * STRIP)

        @pl.when(turn == 0)
        def _():
            for h in range(2):
                for t in range(3):
                    there = outs[t].at[2 * pair + h, pl.ds(0, tokens - 2 * own)]
                    pltpu.make_async_copy(there, there, qkv_recv.at[t, 2 * pair + h]).wait()

        @pl.when(i == 4)
        def _():
            lax.fori_loop(0, 4, lambda n, _: give(0, n), None)

        for n in range(4):
            top_s[n : n + 1, :] = jnp.full((1, STRIP), NEG, jnp.float32)
            mix_s[n] = jnp.zeros(mix_s.shape[1:], jnp.float32)

        def read(ref, h, at):
            return lambda: ref[2 * pair + h, pl.ds(pl.multiple_of(at, STRIP), STRIP), :]

        def whole(b, _):
            at = b * 2 * STRIP
            update([(2 * h + st, read(q_s, h, first + st * STRIP),
                     [(read(k_s, h, at + m * STRIP), read(v_s, h, at + m * STRIP), None) for m in range(2)])
                    for h in range(2) for st in range(2)])

        lax.fori_loop(0, s, whole, None)
        seen = lax.broadcasted_iota(jnp.int32, (STRIP, STRIP), 1) >= lax.broadcasted_iota(jnp.int32, (STRIP, STRIP), 0)
        update([(2 * h + st, read(q_s, h, first + st * STRIP),
                 [(read(k_s, h, first + m * STRIP), read(v_s, h, first + m * STRIP), seen if m == st else None) for m in range(st + 1)])
                for h in range(2) for st in range(2)])

        for h in range(2):
            for st in range(2):
                n = 2 * h + st
                o = (mix_s[n, :HEAD, :] * (1 / mix_s[n, HEAD : HEAD + 1, :])).T.astype(jnp.bfloat16)
                at = pl.ds(pl.multiple_of(first + st * STRIP, STRIP), STRIP)
                @pl.when(2 * s + st == me)
                def _():
                    o_s[:, place(pair, turn, h)] = o

                @pl.when(2 * s + st != me)
                def _():
                    q_s[2 * pair + h, at, :] = o

        @pl.when(pair == 1)
        def _():
            give(1, turn)

    lax.fori_loop(0, 8, attend, None)

    def returned(pair, piece):
        here = o_s.at[:, pl.ds((pair * 8 + piece) * group, group // 2 if piece in (2, 3) else group)]
        pltpu.make_async_copy(here, here, o_recv.at[pair, piece]).wait()

    def out_copy(n):
        lanes = pl.ds(pl.multiple_of(n * W, W), W)
        return pltpu.make_async_copy(a_s.at[pl.ds(own, own), lanes], out_hbm.at[:, lanes], out_sem)

    def finish(part, n, _):
        lane, own_pieces = parts[part]
        depth = len(own_pieces) * group
        bank, at = wo_tile(n)
        wide = wides[part]
        here = w_s.at[bank, at, pl.ds(0, wide * depth)]
        pltpu.make_async_copy(here, here, w_sem.at[bank, at]).wait()
        for c in range(wide):
            to = (n - starts[part]) * wide + c
            y = jnp.dot(o_s[:, lane : lane + depth], w_s[bank, at, c * depth : (c + 1) * depth], preferred_element_type=jnp.float32)
            if part == 0:
                r_s[to] = y
            elif part == 1:
                r_s[to] = r_s[to] + y
            else:
                lanes = pl.ds(pl.multiple_of(to * W, W), W)
                a_s[pl.ds(own, own), lanes] = (a_s[pl.ds(0, own), lanes].astype(jnp.float32) + (r_s[to] + y)).astype(jnp.bfloat16)
        if part == 2:
            for c in range(wide):
                out_copy((n - starts[part]) * wide + c).start()
        for later in range(part, 3):
            @pl.when((n + 6 >= starts[later]) & (n + 6 < starts[later + 1]))
            def _():
                start_wo(n + 6, later)

    x_again.wait()
    for part in range(3):
        for piece in parts[part][1]:
            returned(min(part, 1), piece)
        lax.fori_loop(starts[part], starts[part + 1], lambda n, _, part=part: finish(part, n, _), None)
    pltpu.make_async_copy(a_s.at[pl.ds(own, own)], out_hbm, out_sem).wait()
    pltpu.make_async_copy(stage_s, stage_s, qkv_send).wait()
    sent = q_s.at[:, pl.ds(0, tokens - own)]
    pltpu.make_async_copy(sent, sent, o_send).wait()


def solution(mesh):
    def step(x, gain, wq, wk, wv, wo):
        own, dim = x.shape
        tokens = own * N_DEV
        any_, vmem = pl.BlockSpec(memory_space=pl.ANY), pl.BlockSpec(memory_space=pltpu.VMEM)
        bf16, f32 = jnp.bfloat16, jnp.float32
        dma = pltpu.SemaphoreType.DMA
        heads = pltpu.VMEM((SLOTS, tokens, HEAD), bf16)
        return pl.pallas_call(
            _kernel,
            out_shape=jax.ShapeDtypeStruct((own, dim), bf16),
            in_specs=[any_, vmem, any_, any_, any_, any_],
            out_specs=any_,
            scratch_shapes=[
                pltpu.VMEM((2 * own, HEAD), f32),
                pltpu.VMEM((2 * own, HEAD), f32),
                pltpu.VMEM((2 * own, dim), bf16),
                pltpu.VMEM((2, 3, dim, W), bf16),
                pltpu.VMEM((dim // W, own, W), f32),
                pltpu.VMEM((2, SLOTS, 3, 3 * own, HEAD), bf16),
                heads, heads, heads,
                pltpu.VMEM((own, dim), bf16),
                pltpu.VMEM((4, HEAD + 8, STRIP), f32),
                pltpu.VMEM((8, STRIP), f32),
                dma((4, 2)), dma((2, 3)), dma((2,)), dma((2,)), dma, dma((3, SLOTS)), dma, dma((2, 8)), dma,
            ],
            compiler_params=pltpu.CompilerParams(collective_id=0, has_side_effects=True, vmem_limit_bytes=67043328),
        )(x, gain, wq, wk, wv, wo)

    tokens, whole = P(("dp", "sp"), None), P(None, None)
    return jax.shard_map(
        step,
        mesh=mesh,
        in_specs=(tokens, P(None), whole, whole, whole, whole),
        out_specs=tokens,
        check_vma=False,
    )
```
